256 devices in a mesh: ep: 32 (over z_lo, y, x), dp: 8 (over z_hi, core).
Axes of the slice: x: 4, y: 4, z: 8 (z_hi: 4, z_lo: 2; z = z_hi * 2 + z_lo), core: 2. Of those that a mesh axis runs over, the one named last changes fastest.
Arguments:
- tokens: bfloat16 [16384, 2048], P(('dp', 'ep')), parts along dimension 0, may hold values from -6 to 6
- expert_ids: int32 [16384, 8], P(('dp', 'ep')), parts along dimension 0, may hold values from 0 to 31, all different within a row; in each aligned block of 64 rows (0 to 63, 64 to 127, ...) at most 32 rows name the same one
- gate_probs: float32 [16384, 8], P(('dp', 'ep')), parts along dimension 0, may hold values from 0.05 to 1
- w_gate: bfloat16 [32, 2048, 768], P('ep'), may hold values from -0.125 to 0.125
- w_up: bfloat16 [32, 2048, 768], P('ep'), may hold values from -0.125 to 0.125
- w_down: bfloat16 [32, 768, 2048], P('ep'), may hold values from -0.21875 to 0.21875
Outputs:
- combined: bfloat16 [16384, 2048], P(('dp', 'ep')), parts along dimension 0
The draws below stay inside these ranges and needn't reach their ends.
There are 8 independent parts, one for each index of `dp`. The reference program is written for one: setup_inputs(seed, part) draws one part's arguments, and reference() takes and returns one part's arrays. A program takes and returns all parts, laid end to end along the dimension named above; an argument that names none is the same for every part. Nothing has to cross between parts.
Inputs may be any that keep to these rules, and one draw needn't show every extreme that they name: `expert_ids`: each row names 8 different experts. Among the rows of one index of ep (aligned blocks of 64 rows) no expert is named by more than 32 rows, and in every draw some expert is named by exactly 32 rows of some block. Expert popularity is skewed.
All inputs are finite; a program needn't handle non-finite values.
Results may differ from the reference program's by a relative error of at most 0.0085.
Values may be sent and summed in bfloat16 or wider, within the bound.
No kernel may reach another device: no remote copies, remote signals or barrier semaphores. Data moves between devices by JAX's collectives and lax.ppermute only.
A program may use at most 64 MiB of HBM per device.

```python
import math
import jax
import jax.numpy as jnp
import numpy as np
from jax import lax

D = 2048
FF = 768
TOP = 8
TOK_DEV = 64
EXPERTS = 32
TOKENS = 2048
MOST = 32
N_EP = 32


def levels(key, extent, cuts, least, top_value):
    factor_of, own = 1.0, jax.random.fold_in(key, 6)
    for dim, blocks in cuts:
        steps = jnp.exp(jax.random.uniform(jax.random.fold_in(own, dim), (blocks,), jnp.float32, least / len(cuts), top_value / len(cuts)))
        factor_of = factor_of * jnp.repeat(steps, extent[dim] // blocks).reshape([-1 if axis == dim else 1 for axis in range(len(extent))])
    return factor_of


def deal_out(own_key, own, number, rows, count, top, reach, lean):
    sequence = jax.random.permutation(own_key, count)
    crowded, usual = shares(count, rows * top, reach, lean, True), shares(count, rows * top, reach, lean, False)
    places = jnp.arange(count)

    def named(lengths, offset_by):
        used = int((lengths > 0).sum())
        fixed = max(1, used // 4)
        passed = fixed + (places - fixed + offset_by * (used - fixed)) % max(1, count - fixed)
        return jnp.zeros((count,), jnp.int32).at[sequence[jnp.where(places < fixed, places, passed)]].set(jnp.asarray(lengths, jnp.int32))

    lengths = jnp.where(number % 4 == 0, named(crowded, number // 4), named(usual, number - number // 4 - 1))
    mixed = jax.random.permutation(jax.random.fold_in(own, 3), count)
    source_of, receiver = mixed[0:count // 2 * 2:2], mixed[1:count // 2 * 2:2]
    margin = jnp.minimum(lengths[source_of] - 1, reach - lengths[receiver]) // 2
    margin = jnp.where((source_of == sequence[0]) | (receiver == sequence[0]) | (lengths[receiver] == 0), 0, jnp.maximum(margin, 0))
    passed = jax.random.randint(jax.random.fold_in(own, 4), (count // 2,), 0, 1 << 20) % (margin + 1)
    lengths = lengths.at[source_of].add(-passed).at[receiver].add(passed)
    labels = jnp.searchsorted(jnp.cumsum(lengths), jnp.arange(rows * top), side="right").astype(jnp.int32)
    grid = labels.reshape(top, rows).T
    grid = grid[jax.random.permutation(jax.random.fold_in(own, 1), rows)]
    offset_by = jax.random.randint(jax.random.fold_in(own, 2), (rows, 1), 0, top)
    return jnp.take_along_axis(grid, (jnp.arange(top)[None, :] + offset_by) % top, axis=1)


def shares(amount, total, limit, skew, full):
    loads = [(1 << 20) // math.isqrt(standing ** skew) + 1 for standing in range(1, amount + 1)]
    largest = limit if full else min(limit, max(-(-total // amount), total * loads[0] // sum(loads)))
    least = 1 if total - largest >= amount - 1 else 0
    given, rest = [largest] + [least] * (amount - 1), total - largest - least * (amount - 1)
    while rest > 0:
        movable = [i for i in range(1, amount) if given[i] < largest] or [i for i in range(1, amount) if given[i] < limit]
        mass, left = sum([loads[i] for i in movable]), rest
        for i in movable:
            extra = min(limit - given[i], max(1, left * loads[i] // mass), rest)
            given[i] = given[i] + extra
            rest = rest - extra
    return np.array(given)


def gaussian(own_key, shape, deviation, limit, cuts=(), kind=jnp.bfloat16):
    level = levels(own_key, shape, cuts, -0.22, 0.18) if cuts else 1.0
    values = jax.random.normal(own_key, shape, jnp.float32) * deviation * level
    return jnp.minimum(jnp.maximum(values, -limit), limit).astype(kind)


def setup_inputs(seed: int = 0, part: int = 0) -> dict:
    arg_keys = jax.random.split(jax.random.key(seed), 7)
    part_keys = jax.random.split(jax.random.fold_in(arg_keys[6], part), 7)
    tokens = gaussian(part_keys[0], (TOKENS, D), 1.0, 6.0, ((0, 32),))
    expert_ids_keys = jax.random.split(jax.random.fold_in(part_keys[1], 1), TOKENS // TOK_DEV)
    expert_ids_turns = jax.random.permutation(jax.random.fold_in(part_keys[1], 3), TOKENS // TOK_DEV)
    expert_ids = jax.vmap(lambda own, number: deal_out(jax.random.fold_in(part_keys[1], 2), own, number, TOK_DEV, EXPERTS, TOP, MOST, 2))(expert_ids_keys, expert_ids_turns).reshape((TOKENS, TOP))
    gate_probs = jnp.clip(0.05 + 0.95 * jax.random.uniform(part_keys[2], (TOKENS, TOP), jnp.float32) ** levels(part_keys[2], (TOKENS, TOP), ((0, 32),), -0.2, 0.2), 0.05, 1.0)
    w_gate = gaussian(arg_keys[3], (EXPERTS, D, FF), D ** -0.5, 0.125, ((0, 32),))
    w_up = gaussian(arg_keys[4], (EXPERTS, D, FF), D ** -0.5, 0.125, ((0, 32),))
    w_down = gaussian(arg_keys[5], (EXPERTS, FF, D), FF ** -0.5, 0.21875, ((0, 32),))
    return dict(tokens=tokens, expert_ids=expert_ids, gate_probs=gate_probs, w_gate=w_gate, w_up=w_up, w_down=w_down)


def expert_ffn(row_block, gate_matrix, up_matrix, down_matrix):
    gate_act = jnp.dot(row_block, gate_matrix, preferred_element_type=jnp.float32)
    up_act = jnp.dot(row_block, up_matrix, preferred_element_type=jnp.float32)
    hidden = (jax.nn.silu(gate_act) * up_act).astype(jnp.bfloat16)
    return jnp.dot(hidden, down_matrix, preferred_element_type=jnp.float32).astype(jnp.bfloat16)


def reference(tokens, expert_ids, gate_probs, w_gate, w_up, w_down):
    experts = w_gate.shape[0]
    capacity = N_EP * MOST
    flat_ids = expert_ids.reshape(-1).astype(jnp.int32)
    owners = (jnp.arange(flat_ids.shape[0], dtype=jnp.int32) // TOP).astype(jnp.int32)
    onehot = (flat_ids[:, None] == jnp.arange(experts, dtype=jnp.int32)[None, :]).astype(jnp.int32)
    within_rank = jnp.sum((jnp.cumsum(onehot, axis=0) - onehot) * onehot, axis=1).astype(jnp.int32)
    slot_index = (flat_ids * capacity + within_rank).astype(jnp.int32)
    slot_token = jnp.zeros((experts * capacity,), jnp.int32).at[slot_index].set(owners)
    filled = jnp.zeros((experts * capacity,), jnp.bool_).at[slot_index].set(True)

    def per_expert(expert_index):
        row_start = (expert_index * capacity).astype(jnp.int32)
        chosen = lax.dynamic_slice_in_dim(slot_token, row_start, capacity, 0)
        present = lax.dynamic_slice_in_dim(filled, row_start, capacity, 0)
        row_block = jnp.where(present[:, None], tokens[chosen], jnp.zeros((), jnp.bfloat16))
        return expert_ffn(row_block, w_gate[expert_index], w_up[expert_index], w_down[expert_index])

    outputs = lax.map(per_expert, jnp.arange(experts, dtype=jnp.int32))
    picked = outputs.reshape(-1, tokens.shape[1])[slot_index].astype(jnp.float32)
    picked = picked.reshape(tokens.shape[0], TOP, tokens.shape[1])
    weights = gate_probs / jnp.sum(gate_probs, axis=1, keepdims=True)
    combined = jnp.sum(picked * weights[:, :, None], axis=1)
    return combined.astype(jnp.bfloat16)
```

```python
import functools

import jax
import jax.numpy as jnp
from jax import lax
from jax.experimental import pallas as pl
from jax.experimental.pallas import tpu as pltpu
from jax.sharding import Mesh, PartitionSpec as P


F32 = jnp.float32
BF16 = jnp.bfloat16
CAP = 32
SIDE = 4
META = 128
VMEM = pl.BlockSpec(memory_space=pltpu.VMEM)
PARAMS = pltpu.CompilerParams(vmem_limit_bytes=48 * 1024 * 1024)


def prep_kernel(tok_ref, ids_ref, prob_ref, out_ref):
    half = tok_ref.shape[1] // 2
    top = ids_ref.shape[1]
    prob = prob_ref[...]
    weight = prob / jnp.sum(prob, axis=1, keepdims=True)
    high = weight.astype(BF16)
    low = (weight - high.astype(F32)).astype(BF16)
    row = lax.broadcasted_iota(jnp.int32, (top, META), 0)
    lane = lax.broadcasted_iota(jnp.int32, (top, META), 1)
    meta = jnp.zeros((tok_ref.shape[0], META), F32)
    for place, piece in enumerate((ids_ref[...].astype(F32).astype(BF16), high, low)):
        spread = (lane == row + place * top).astype(F32).astype(BF16)
        meta = meta + jnp.dot(piece, spread, preferred_element_type=F32)
    meta = meta.astype(BF16)
    for side in range(2):
        out_ref[side, :, :half] = tok_ref[:, side * half : (side + 1) * half]
        out_ref[side, :, half:] = meta


def pack_kernel(top, owners_ref, first_ref, *refs):
    others, outs, weights_ref = refs[:6], refs[6:14], refs[14]
    rows = first_ref.shape[1]
    half = first_ref.shape[2] - META
    slots = SIDE * CAP
    lane = lax.broadcasted_iota(jnp.int32, (rows, slots), 1)
    slot = (lane % CAP).astype(F32)
    before = (
        lax.broadcasted_iota(jnp.int32, (rows, rows), 0) > lax.broadcasted_iota(jnp.int32, (rows, rows), 1)
    ).astype(F32).astype(BF16)
    for side in range(2):
        owner = owners_ref[side : side + 1, :]
        for block in range(SIDE):
            ref = first_ref.at[side] if block == 0 else others[side * 3 + block - 1]
            meta = ref[:, half:].astype(F32)
            named = jnp.zeros((rows, slots), F32)
            weight_high = jnp.zeros((rows, slots), F32)
            weight_low = jnp.zeros((rows, slots), F32)
            for k in range(top):
                hit = meta[:, k : k + 1] == owner
                named = jnp.where(hit, 1.0, named)
                weight_high = jnp.where(hit, meta[:, top + k : top + k + 1], weight_high)
                weight_low = jnp.where(hit, meta[:, 2 * top + k : 2 * top + k + 1], weight_low)
            rank = jnp.dot(before, named.astype(BF16), preferred_element_type=F32)
            chosen = jnp.where(rank == slot, named, 0.0)
            picked = lax.dot_general(
                chosen.astype(BF16), ref[:, :half], (((0,), (0,)), ((), ())), preferred_element_type=F32
            ).astype(BF16)
            for d in range(SIDE):
                outs[side * SIDE + d][block * CAP : (block + 1) * CAP, :] = picked[d * CAP : (d + 1) * CAP, :]
            weights_ref[side * SIDE + block, :, :slots] = (chosen * weight_high).astype(BF16)
            weights_ref[side * SIDE + block, :, slots:] = (chosen * weight_low).astype(BF16)


def unpack_kernel(weights_ref, *refs):
    rows_in, outs = refs[:8], refs[8:16]
    for side in range(2):
        for block in range(SIDE):
            stacked = jnp.concatenate(
                [rows_in[side * SIDE + d][block * CAP : (block + 1) * CAP, :] for d in range(SIDE)], axis=0
            )
            weights = weights_ref[side * SIDE + block]
            slots = SIDE * CAP
            total = jnp.dot(weights[:, :slots], stacked, preferred_element_type=F32)
            total = total + jnp.dot(weights[:, slots:], stacked, preferred_element_type=F32)
            outs[side * SIDE + block][...] = total.astype(BF16)


def call(kernel, shapes, *args):
    return pl.pallas_call(
        kernel,
        out_shape=shapes,
        in_specs=[VMEM] * len(args),
        out_specs=jax.tree.map(lambda _: VMEM, shapes),
        compiler_params=PARAMS,
    )(*args)


def shift(value, axis, by):
    count = lax.axis_size(axis)
    return lax.ppermute(value, axis, [(i, (i + by) % count) for i in range(count)])


def ffn(a_rows, b_rows, w_gate, w_up, w_down):
    half = a_rows[0].shape[1]
    a = jnp.stack([r.reshape(SIDE, CAP, half) for r in a_rows], axis=1).reshape(-1, half)
    b = jnp.stack([r.reshape(SIDE, CAP, half) for r in b_rows], axis=0).reshape(-1, half)
    rows = jnp.concatenate([a, b], axis=1)
    gate = jnp.dot(rows, w_gate, preferred_element_type=F32)
    up = jnp.dot(rows, w_up, preferred_element_type=F32)
    hidden = (jax.nn.silu(gate) * up).astype(BF16)
    out = jnp.dot(hidden, w_down, preferred_element_type=F32).astype(BF16)
    out = out.reshape(SIDE, SIDE, CAP, 2 * half)
    a_out = [out[:, d, :, :half].reshape(-1, half) for d in range(SIDE)]
    b_out = [out[d, :, :, half:].reshape(-1, half) for d in range(SIDE)]
    return a_out, b_out


STEPS = (2, 1, 3)


def spread(both):
    got = {}
    for d in STEPS:
        got[0, d] = shift(both[0], "y", d)
        got[1, d] = shift(both[1], "x", d)
    return [got[side, d] for side in range(2) for d in (1, 2, 3)]


def send(packed):
    a, b = [packed[0]] + [None] * 3, [packed[4]] + [None] * 3
    for d in STEPS:
        a[d] = shift(packed[d], "x", d)
        b[d] = shift(packed[4 + d], "y", d)
    return a, b


def send_back(a_out, b_out):
    a, b = [a_out[0]] + [None] * 3, [b_out[0]] + [None] * 3
    for d in STEPS:
        a[d] = shift(a_out[d], "x", -d)
        b[d] = shift(b_out[d], "y", -d)
    return a + b


def gather_back(partial):
    a, b = [partial[0]] + [None] * 3, [partial[4]] + [None] * 3
    for d in STEPS:
        a[d] = shift(partial[d], "y", -d)
        b[d] = shift(partial[4 + d], "x", -d)
    total = lambda parts: sum(p.astype(F32) for p in parts)
    return jnp.concatenate([total(a), total(b)], axis=1)


def shards(tokens, expert_ids, gate_probs, w_gate, w_up, w_down):
    count, features = tokens.shape
    half = features // 2
    top = expert_ids.shape[1]
    z, y, x = (lax.axis_index(n) for n in "zyx")
    step = jnp.arange(SIDE * CAP, dtype=jnp.int32) // CAP
    base = z * SIDE * SIDE
    owners = jnp.stack([base + y * SIDE + (x + step) % SIDE, base + (y + step) % SIDE * SIDE + x]).astype(F32)
    shape = jax.ShapeDtypeStruct

    mine = call(prep_kernel, shape((2, count, half + META), BF16), tokens, expert_ids, gate_probs)
    theirs = shift(mine, "z", 1)
    pack_shapes = [shape((SIDE * CAP, half), BF16)] * 8 + [shape((8, count, 2 * SIDE * CAP), BF16)]
    unpack_shapes = [shape((count, half), BF16)] * 8
    w = (w_gate[0], w_up[0], w_down[0])

    packs = []
    for both in (mine, theirs):
        packs.append(call(functools.partial(pack_kernel, top), pack_shapes, owners, both, *spread(both)))
    arrived = [send(p[:8]) for p in packs]
    served = [send_back(*ffn(*a, *w)) for a in arrived]
    partial = [call(unpack_kernel, unpack_shapes, p[8], *s) for p, s in zip(packs, served)]
    other = gather_back(partial[1]).astype(BF16)
    back = shift(other, "z", 1)
    own = gather_back(partial[0])
    return (own + back.astype(F32)).astype(BF16)


def solution(mesh):
    grid = Mesh(mesh.devices.reshape(2, SIDE, SIDE, 4, 2), ("z", "y", "x", "h", "c"))
    rows = P(("h", "c", "z", "y", "x"), None)
    owner = P(("z", "y", "x"), None, None)
    return jax.shard_map(
        shards, mesh=grid, in_specs=(rows, rows, rows, owner, owner, owner), out_specs=rows, check_vma=False
    )
```

```python
import jax
import jax.numpy as jnp
from jax import lax
from jax.experimental import pallas as pl
from jax.experimental.pallas import tpu as pltpu
from jax.sharding import Mesh, PartitionSpec as P


F32 = jnp.float32
BF16 = jnp.bfloat16
CAP = 32
SIDE = 4
EXPERTS = 32
META = 128
SLOTS = SIDE * CAP
NONE = 255.0
VMEM = pl.BlockSpec(memory_space=pltpu.VMEM)
PARAMS = pltpu.CompilerParams(vmem_limit_bytes=48 * 1024 * 1024)


def prep_kernel(tok_ref, ids_ref, prob_ref, out_ref):
    rows, features = tok_ref.shape
    top = ids_ref.shape[0]
    out_ref[:, :features] = tok_ref[...]
    prob = prob_ref[...]
    weight = (prob / jnp.sum(prob, axis=0, keepdims=True)).T
    ids = ids_ref[...].astype(F32).T
    lane = lax.broadcasted_iota(jnp.int32, (rows, META), 1)
    expert = (lane % EXPERTS).astype(F32)
    named = jnp.zeros((rows, META), F32)
    value = jnp.zeros((rows, META), F32)
    for k in range(top):
        hit = ids[:, k : k + 1] == expert
        named = jnp.where(hit, 1.0, named)
        value = jnp.where(hit, weight[:, k : k + 1], value)
    before = (
        lax.broadcasted_iota(jnp.int32, (rows, rows), 0) > lax.broadcasted_iota(jnp.int32, (rows, rows), 1)
    ).astype(F32).astype(BF16)
    rank = jnp.dot(before, named.astype(BF16), preferred_element_type=F32)
    slot = jnp.where(named > 0.0, rank, NONE)
    high = value.astype(BF16).astype(F32)
    part = lane // EXPERTS
    meta = jnp.where(part == 0, slot, jnp.where(part == 1, high, value - high))
    out_ref[:, features:] = meta.astype(BF16)


def pack_kernel(owner_ref, *refs):
    blocks, outs, weights_ref = refs[:SIDE], refs[SIDE : 2 * SIDE], refs[2 * SIDE]
    rows, width = blocks[0].shape
    features = width - META
    owner = owner_ref[...]
    source = lax.broadcasted_iota(jnp.int32, (META, SLOTS), 0)
    pick = [(source == owner + part * EXPERTS).astype(F32).astype(BF16) for part in range(3)]
    place = (lax.broadcasted_iota(jnp.int32, (rows, SLOTS), 1) % CAP).astype(F32)
    for b in range(SIDE):
        meta = blocks[b][:, features:]
        slot, high, low = (jnp.dot(meta, p, preferred_element_type=F32) for p in pick)
        chosen = slot == place
        weights_ref[b, :, :SLOTS] = jnp.where(chosen, high, 0.0).astype(BF16)
        weights_ref[b, :, SLOTS:] = jnp.where(chosen, low, 0.0).astype(BF16)
        table = jnp.where(chosen, 1.0, 0.0).T.astype(BF16)
        picked = jnp.dot(table, blocks[b][:, :features], preferred_element_type=F32).astype(BF16)
        for d in range(SIDE):
            outs[d][b * CAP : (b + 1) * CAP, :] = picked[d * CAP : (d + 1) * CAP, :]


def unpack_kernel(weights_ref, *refs):
    rows_in, outs = refs[:SIDE], refs[SIDE : 2 * SIDE]
    for b in range(SIDE):
        stacked = jnp.concatenate([r[b * CAP : (b + 1) * CAP, :] for r in rows_in], axis=0)
        total = jnp.dot(weights_ref[b, :, :SLOTS], stacked, preferred_element_type=F32)
        total = total + jnp.dot(weights_ref[b, :, SLOTS:], stacked, preferred_element_type=F32)
        outs[b][...] = total.astype(BF16)


def ffn_kernel(gate_ref, up_ref, down_ref, *refs):
    rows_in, outs, held, hidden = refs[:SIDE], refs[SIDE : 2 * SIDE], refs[2 * SIDE], refs[2 * SIDE + 1]
    height = rows_in[0].shape[0]
    inner = gate_ref.shape[2]
    features = down_ref.shape[2]
    for d in range(SIDE):
        held[d * height : (d + 1) * height, :] = rows_in[d][...]
    tile = 256
    for t in range(inner // tile):
        cols = slice(t * tile, (t + 1) * tile)
        gate = jnp.dot(held[...], gate_ref[0, :, cols], preferred_element_type=F32)
        up = jnp.dot(held[...], up_ref[0, :, cols], preferred_element_type=F32)
        hidden[:, cols] = (gate / (1.0 + jnp.exp(-gate)) * up).astype(BF16)
    for t in range(features // tile):
        cols = slice(t * tile, (t + 1) * tile)
        out = jnp.dot(hidden[...], down_ref[0, :, cols], preferred_element_type=F32).astype(BF16)
        for d in range(SIDE):
            outs[d][:, cols] = out[d * height : (d + 1) * height, :]


def call(kernel, shapes, *args, scratch=()):
    return pl.pallas_call(
        kernel,
        out_shape=shapes,
        in_specs=[VMEM] * len(args),
        out_specs=jax.tree.map(lambda _: VMEM, shapes),
        scratch_shapes=scratch,
        compiler_params=PARAMS,
    )(*args)


STEPS = (1, 3, 2)


def shift(value, axis, by):
    count = lax.axis_size(axis)
    return lax.ppermute(value, axis, [(i, (i + by) % count) for i in range(count)])


def shift_all(values, axis, sign):
    out = [values[0]] + [None] * (SIDE - 1)
    for d in STEPS:
        out[d] = shift(values[d], axis, sign * d)
    return out


def shards(tokens, expert_ids, gate_probs, w_gate, w_up, w_down):
    count, features = tokens.shape
    inner = w_gate.shape[2]
    z, y, x = (lax.axis_index(n) for n in "zyx")
    step = (jnp.arange(SLOTS, dtype=jnp.int32) // CAP)[None, :]
    base = z * SIDE * SIDE
    owners = (base + y * SIDE + (x + step) % SIDE, base + (y + step) % SIDE * SIDE + x)
    shape = jax.ShapeDtypeStruct

    mine = call(prep_kernel, shape((count, features + META), BF16), tokens, expert_ids.T, gate_probs.T)
    theirs = shift(mine, "z", 1)
    pack_shapes = [shape((SLOTS, features), BF16)] * SIDE + [shape((SIDE, count, 2 * SLOTS), BF16)]
    unpack_shapes = [shape((count, features), BF16)] * SIDE
    ffn_shapes = [shape((SLOTS, features), BF16)] * SIDE
    height = SIDE * SLOTS
    scratch = [pltpu.VMEM((height, features), BF16), pltpu.VMEM((height, inner), BF16)]

    axes = (("y", "x"), ("x", "y"))
    gathered = [shift_all([b] * SIDE, first, 1) for b, (first, _) in zip((mine, theirs), axes)]
    packs = [call(pack_kernel, pack_shapes, o, *g) for o, g in zip(owners, gathered)]
    arrived = [shift_all(p[:SIDE], last, 1) for p, (_, last) in zip(packs, axes)]
    served = [call(ffn_kernel, ffn_shapes, w_gate, w_up, w_down, *a, scratch=scratch) for a in arrived]
    back = [shift_all(s, last, -1) for s, (_, last) in zip(served, axes)]
    partial = [call(unpack_kernel, unpack_shapes, p[SIDE], *b) for p, b in zip(packs, back)]
    total = lambda parts: sum(p.astype(F32) for p in parts)
    other = total(shift_all(partial[1], "x", -1)).astype(BF16)
    own = total(shift_all(partial[0], "y", -1))
    return (own + shift(other, "z", 1).astype(F32)).astype(BF16)


def solution(mesh):
    grid = Mesh(mesh.devices.reshape(2, SIDE, SIDE, 4, 2), ("z", "y", "x", "h", "c"))
    rows = P(("h", "c", "z", "y", "x"), None)
    owner = P(("z", "y", "x"), None, None)
    return jax.shard_map(
        shards, mesh=grid, in_specs=(rows, rows, rows, owner, owner, owner), out_specs=rows, check_vma=False
    )
```

```python
import jax
import jax.numpy as jnp
from jax import lax
from jax.experimental import pallas as pl
from jax.experimental.pallas import tpu as pltpu
from jax.sharding import Mesh, PartitionSpec as P


F32 = jnp.float32
BF16 = jnp.bfloat16
CAP = 32
SIDE = 4
EXPERTS = 32
META = 128
SLOTS = SIDE * CAP
NONE = 255.0
VMEM = pl.BlockSpec(memory_space=pltpu.VMEM)
PARAMS = pltpu.CompilerParams(vmem_limit_bytes=48 * 1024 * 1024)


def prep_kernel(tok_hbm, ids_hbm, prob_hbm, out_ref, ids_ref, prob_ref, sems):
    rows, features = tok_hbm.shape
    top = ids_hbm.shape[0]
    pairs = ((ids_hbm, ids_ref), (prob_hbm, prob_ref), (tok_hbm, out_ref.at[:, :features]))
    copies = [pltpu.make_async_copy(a, b, sems.at[i]) for i, (a, b) in enumerate(pairs)]
    for copy in copies:
        copy.start()
    copies[0].wait()
    copies[1].wait()
    prob = prob_ref[...]
    weight = (prob / jnp.sum(prob, axis=0, keepdims=True)).T
    ids = ids_ref[...].astype(F32).T
    lane = lax.broadcasted_iota(jnp.int32, (rows, META), 1)
    expert = (lane % EXPERTS).astype(F32)
    named = jnp.zeros((rows, META), F32)
    value = jnp.zeros((rows, META), F32)
    for k in range(top):
        hit = ids[:, k : k + 1] == expert
        named = jnp.where(hit, 1.0, named)
        value = jnp.where(hit, weight[:, k : k + 1], value)
    before = (
        lax.broadcasted_iota(jnp.int32, (rows, rows), 0) > lax.broadcasted_iota(jnp.int32, (rows, rows), 1)
    ).astype(F32).astype(BF16)
    rank = jnp.dot(before, named.astype(BF16), preferred_element_type=F32)
    slot = jnp.where(named > 0.0, rank, NONE)
    high = value.astype(BF16).astype(F32)
    part = lane // EXPERTS
    meta = jnp.where(part == 0, slot, jnp.where(part == 1, high, value - high))
    out_ref[:, features:] = meta.astype(BF16)
    copies[2].wait()


def pack_kernel(owner_ref, *refs):
    blocks, outs, weights_ref = refs[:SIDE], refs[SIDE : 2 * SIDE], refs[2 * SIDE]
    rows, width = blocks[0].shape
    features = width - META
    owner = owner_ref[...]
    source = lax.broadcasted_iota(jnp.int32, (META, SLOTS), 0)
    pick = [(source == owner + part * EXPERTS).astype(F32).astype(BF16) for part in range(3)]
    place = (lax.broadcasted_iota(jnp.int32, (rows, SLOTS), 1) % CAP).astype(F32)
    for b in range(SIDE):
        meta = blocks[b][:, features:]
        slot, high, low = (jnp.dot(meta, p, preferred_element_type=F32) for p in pick)
        chosen = slot == place
        weights_ref[b, :, :SLOTS] = jnp.where(chosen, high, 0.0).astype(BF16)
        weights_ref[b, :, SLOTS:] = jnp.where(chosen, low, 0.0).astype(BF16)
        table = jnp.where(chosen, 1.0, 0.0).T.astype(BF16)
        picked = jnp.dot(table, blocks[b][:, :features], preferred_element_type=F32).astype(BF16)
        for d in range(SIDE):
            outs[d][b * CAP : (b + 1) * CAP, :] = picked[d * CAP : (d + 1) * CAP, :]


def unpack_kernel(weights_ref, *refs):
    rows_in, outs = refs[:SIDE], refs[SIDE : 2 * SIDE]
    for b in range(SIDE):
        stacked = jnp.concatenate([r[b * CAP : (b + 1) * CAP, :] for r in rows_in], axis=0)
        total = jnp.dot(weights_ref[b, :, :SLOTS], stacked, preferred_element_type=F32)
        total = total + jnp.dot(weights_ref[b, :, SLOTS:], stacked, preferred_element_type=F32)
        outs[b][...] = total.astype(BF16)


def ffn_kernel(gate_ref, up_ref, down_ref, *refs):
    rows_in, outs, held, hidden = refs[:SIDE], refs[SIDE : 2 * SIDE], refs[2 * SIDE], refs[2 * SIDE + 1]
    height = rows_in[0].shape[0]
    inner = gate_ref.shape[2]
    features = down_ref.shape[2]
    for d in range(SIDE):
        held[d * height : (d + 1) * height, :] = rows_in[d][...]
    tile = 256
    for t in range(inner // tile):
        cols = slice(t * tile, (t + 1) * tile)
        gate = jnp.dot(held[...], gate_ref[0, :, cols], preferred_element_type=F32)
        up = jnp.dot(held[...], up_ref[0, :, cols], preferred_element_type=F32)
        hidden[:, cols] = (gate / (1.0 + jnp.exp(-gate)) * up).astype(BF16)
    for t in range(features // tile):
        cols = slice(t * tile, (t + 1) * tile)
        out = jnp.dot(hidden[...], down_ref[0, :, cols], preferred_element_type=F32).astype(BF16)
        for d in range(SIDE):
            outs[d][:, cols] = out[d * height : (d + 1) * height, :]


def call(kernel, shapes, *args, scratch=(), space=pltpu.VMEM):
    return pl.pallas_call(
        kernel,
        out_shape=shapes,
        in_specs=[pl.BlockSpec(memory_space=space)] * len(args),
        out_specs=jax.tree.map(lambda _: VMEM, shapes),
        scratch_shapes=scratch,
        compiler_params=PARAMS,
    )(*args)


STEPS = (1, 3, 2)


def shift(value, axis, by):
    count = lax.axis_size(axis)
    return lax.ppermute(value, axis, [(i, (i + by) % count) for i in range(count)])


def shift_all(values, axis, sign):
    out = [values[0]] + [None] * (SIDE - 1)
    for d in STEPS:
        out[d] = shift(values[d], axis, sign * d)
    return out


def shards(tokens, expert_ids, gate_probs, w_gate, w_up, w_down):
    count, features = tokens.shape
    top = expert_ids.shape[1]
    inner = w_gate.shape[2]
    z, y, x = (lax.axis_index(n) for n in "zyx")
    step = (jnp.arange(SLOTS, dtype=jnp.int32) // CAP)[None, :]
    base = z * SIDE * SIDE
    owners = (base + y * SIDE + (x + step) % SIDE, base + (y + step) % SIDE * SIDE + x)
    shape = jax.ShapeDtypeStruct

    mine = call(
        prep_kernel, shape((count, features + META), BF16), tokens, expert_ids.T, gate_probs.T,
        space=pltpu.HBM,
        scratch=[pltpu.VMEM((top, count), jnp.int32), pltpu.VMEM((top, count), F32), pltpu.SemaphoreType.DMA((3,))],
    )
    theirs = shift(mine, "z", 1)
    pack_shapes = [shape((SLOTS, features), BF16)] * SIDE + [shape((SIDE, count, 2 * SLOTS), BF16)]
    unpack_shapes = [shape((count, features), BF16)] * SIDE
    ffn_shapes = [shape((SLOTS, features), BF16)] * SIDE
    height = SIDE * SLOTS
    scratch = [pltpu.VMEM((height, features), BF16), pltpu.VMEM((height, inner), BF16)]

    partial = []
    for block, owner, first, last in ((mine, owners[0], "y", "x"), (theirs, owners[1], "x", "y")):
        gathered = shift_all([block] * SIDE, first, 1)
        *packed, weights = call(pack_kernel, pack_shapes, owner, *gathered)
        arrived = shift_all(packed, last, 1)
        served = call(ffn_kernel, ffn_shapes, w_gate, w_up, w_down, *arrived, scratch=scratch)
        back = shift_all(served, last, -1)
        summed = call(unpack_kernel, unpack_shapes, weights, *back)
        partial.append(sum(p.astype(F32) for p in shift_all(summed, first, -1)))
    own, other = partial
    return (own + shift(other.astype(BF16), "z", 1).astype(F32)).astype(BF16)


def solution(mesh):
    grid = Mesh(mesh.devices.reshape(2, SIDE, SIDE, 4, 2), ("z", "y", "x", "h", "c"))
    rows = P(("h", "c", "z", "y", "x"), None)
    owner = P(("z", "y", "x"), None, None)

    return jax.shard_map(
        shards, mesh=grid, in_specs=(rows, rows, rows, owner, owner, owner), out_specs=rows, check_vma=False
    )
```

```python
import jax
import jax.numpy as jnp
from jax import lax
from jax.experimental import pallas as pl
from jax.experimental.pallas import tpu as pltpu
from jax.sharding import Mesh, PartitionSpec as P


F32 = jnp.float32
BF16 = jnp.bfloat16
CAP = 32
SIDE = 4
EXPERTS = 32
META = 128
SLOTS = SIDE * CAP
NONE = 255.0
VMEM = pl.BlockSpec(memory_space=pltpu.VMEM)


def prep_kernel(tok_ref, table_ref, out_ref):
    rows, features = tok_ref.shape
    top = table_ref.shape[0] // 2
    out_ref[:, :features] = tok_ref[...]
    table = table_ref[...].T
    ids, weight = table[:, :top], table[:, top:]
    lane = lax.broadcasted_iota(jnp.int32, (rows, META), 1)
    expert = (lane % EXPERTS).astype(F32)
    named = jnp.zeros((rows, META), F32)
    value = jnp.zeros((rows, META), F32)
    for k in range(top):
        hit = ids[:, k : k + 1] == expert
        named = jnp.where(hit, 1.0, named)
        value = jnp.where(hit, weight[:, k : k + 1], value)
    before = (
        lax.broadcasted_iota(jnp.int32, (rows, rows), 0) > lax.broadcasted_iota(jnp.int32, (rows, rows), 1)
    ).astype(F32).astype(BF16)
    rank = jnp.dot(before, named.astype(BF16), preferred_element_type=F32)
    slot = jnp.where(named > 0.0, rank, NONE)
    high = value.astype(BF16).astype(F32)
    part = lane // EXPERTS
    meta = jnp.where(part == 0, slot, jnp.where(part == 1, high, value - high))
    out_ref[:, features:] = meta.astype(BF16)


def pack_kernel(owner_ref, *refs):
    blocks, outs, weights_ref = refs[:SIDE], refs[SIDE : 2 * SIDE], refs[2 * SIDE]
    rows, width = blocks[0].shape
    features = width - META
    owner = owner_ref[...]
    source = lax.broadcasted_iota(jnp.int32, (META, SLOTS), 0)
    pick = [(source == owner + part * EXPERTS).astype(F32).astype(BF16) for part in range(3)]
    place = (lax.broadcasted_iota(jnp.int32, (rows, SLOTS), 1) % CAP).astype(F32)
    for b in range(SIDE):
        meta = blocks[b][:, features:]
        slot, high, low = (jnp.dot(meta, p, preferred_element_type=F32) for p in pick)
        chosen = slot == place
        weights_ref[b, :, :SLOTS] = jnp.where(chosen, high, 0.0).astype(BF16)
        weights_ref[b, :, SLOTS:] = jnp.where(chosen, low, 0.0).astype(BF16)
        table = jnp.where(chosen, 1.0, 0.0).T.astype(BF16)
        picked = jnp.dot(table, blocks[b][:, :features], preferred_element_type=F32).astype(BF16)
        for d in range(SIDE):
            outs[d][b * CAP : (b + 1) * CAP, :] = picked[d * CAP : (d + 1) * CAP, :]


def unpack_kernel(weights_ref, *refs):
    rows_in, outs = refs[:SIDE], refs[SIDE : 2 * SIDE]
    for b in range(SIDE):
        stacked = jnp.concatenate([r[b * CAP : (b + 1) * CAP, :] for r in rows_in], axis=0)
        total = jnp.dot(weights_ref[b, :, :SLOTS], stacked, preferred_element_type=F32)
        total = total + jnp.dot(weights_ref[b, :, SLOTS:], stacked, preferred_element_type=F32)
        outs[b][...] = total.astype(BF16)


def ffn_kernel(gate_ref, up_ref, down_ref, *refs):
    rows_in, outs, held, hidden = refs[:SIDE], refs[SIDE : 2 * SIDE], refs[2 * SIDE], refs[2 * SIDE + 1]
    height = rows_in[0].shape[0]
    inner = gate_ref.shape[2]
    features = down_ref.shape[2]
    for d in range(SIDE):
        held[d * height : (d + 1) * height, :] = rows_in[d][...]
    tile = 256
    for t in range(inner // tile):
        cols = slice(t * tile, (t + 1) * tile)
        gate = jnp.dot(held[...], gate_ref[0, :, cols], preferred_element_type=F32)
        up = jnp.dot(held[...], up_ref[0, :, cols], preferred_element_type=F32)
        hidden[:, cols] = (gate / (1.0 + jnp.exp(-gate)) * up).astype(BF16)
    for t in range(features // tile):
        cols = slice(t * tile, (t + 1) * tile)
        out = jnp.dot(hidden[...], down_ref[0, :, cols], preferred_element_type=F32).astype(BF16)
        for d in range(SIDE):
            outs[d][:, cols] = out[d * height : (d + 1) * height, :]


def call(kernel, shapes, *args, scratch=(), limit=12):
    return pl.pallas_call(
        kernel,
        out_shape=shapes,
        in_specs=[VMEM] * len(args),
        out_specs=jax.tree.map(lambda _: VMEM, shapes),
        scratch_shapes=scratch,
        compiler_params=pltpu.CompilerParams(vmem_limit_bytes=limit * 1024 * 1024),
    )(*args)


STEPS = (1, 3, 2)


def shift(value, axis, by):
    count = lax.axis_size(axis)
    return lax.ppermute(value, axis, [(i, (i + by) % count) for i in range(count)])


def shift_all(values, axis, sign):
    out = [values[0]] + [None] * (SIDE - 1)
    for d in STEPS:
        out[d] = shift(values[d], axis, sign * d)
    return out


def shards(tokens, expert_ids, gate_probs, w_gate, w_up, w_down):
    count, features = tokens.shape
    inner = w_gate.shape[2]
    z, y, x = (lax.axis_index(n) for n in "zyx")
    step = (jnp.arange(SLOTS, dtype=jnp.int32) // CAP)[None, :]
    base = z * SIDE * SIDE
    owners = (base + y * SIDE + (x + step) % SIDE, base + (y + step) % SIDE * SIDE + x)
    shape = jax.ShapeDtypeStruct

    weights = gate_probs / jnp.sum(gate_probs, axis=1, keepdims=True)
    table = jnp.concatenate([expert_ids.astype(F32), weights], axis=1).T
    mine = call(prep_kernel, shape((count, features + META), BF16), tokens, table, limit=8)
    theirs = shift(mine, "z", 1)
    pack_shapes = [shape((SLOTS, features), BF16)] * SIDE + [shape((SIDE, count, 2 * SLOTS), BF16)]
    unpack_shapes = [shape((count, features), BF16)] * SIDE
    ffn_shapes = [shape((SLOTS, features), BF16)] * SIDE
    height = SIDE * SLOTS
    scratch = [pltpu.VMEM((height, features), BF16), pltpu.VMEM((height, inner), BF16)]

    partial = []
    for block, owner, first, last in ((mine, owners[0], "y", "x"), (theirs, owners[1], "x", "y")):
        gathered = shift_all([block] * SIDE, first, 1)
        *packed, weights = call(pack_kernel, pack_shapes, owner, *gathered)
        arrived = shift_all(packed, last, 1)
        served = call(ffn_kernel, ffn_shapes, w_gate, w_up, w_down, *arrived, scratch=scratch, limit=24)
        back = shift_all(served, last, -1)
        summed = call(unpack_kernel, unpack_shapes, weights, *back)
        partial.append(sum(p.astype(F32) for p in shift_all(summed, first, -1)))
    own, other = partial
    return (own + shift(other.astype(BF16), "z", 1).astype(F32)).astype(BF16)


def solution(mesh):
    grid = Mesh(mesh.devices.reshape(2, SIDE, SIDE, 4, 2), ("z", "y", "x", "h", "c"))
    rows = P(("h", "c", "z", "y", "x"), None)
    owner = P(("z", "y", "x"), None, None)

    return jax.shard_map(
        shards, mesh=grid, in_specs=(rows, rows, rows, owner, owner, owner), out_specs=rows, check_vma=False
    )
```
